32 devices in a mesh: dp: 8 (over y, x, core), tensor: 4 (over z).
Axes of the slice: x: 2, y: 2, z: 4, core: 2. Of those that a mesh axis runs over, the one named last changes fastest.
Arguments:
- hidden_in: bfloat16 [8192, 2048], P(('dp', 'tensor')), may hold values from -6 to 6
- qkv_weight: bfloat16 [3, 2048, 2048], P(None, 'dp', 'tensor'), may hold values from -0.125 to 0.125
- head_bias: float32 [3, 2048], P(None, 'tensor'), may hold values from -3 to 3
- dense_weight: bfloat16 [2048, 2048], P('tensor', 'dp'), may hold values from -1 to 1
- dense_bias: float32 [2048], replicated, may hold values from -3 to 3
- fc1_weight: bfloat16 [2048, 8192], P('dp', 'tensor'), may hold values from -0.125 to 0.125
- fc1_bias: float32 [8192], P('tensor'), may hold values from -3 to 3
- fc2_weight: bfloat16 [8192, 2048], P('tensor', 'dp'), may hold values from -0.0625 to 0.0625
- fc2_bias: float32 [2048], replicated, may hold values from -3 to 3
- norm_gain: float32 [2048], replicated, may hold values from 0.5 to 1.5
- norm_bias: float32 [2048], replicated, may hold values from -2 to 2
- out_grad: bfloat16 [8192, 2048], P(('dp', 'tensor')), may hold values from -6 to 6
Outputs:
- hidden_out: bfloat16 [8192, 2048], P(('dp', 'tensor'))
- hidden_grad: bfloat16 [8192, 2048], P(('dp', 'tensor'))
- qkv_weight_grad: float32 [3, 2048, 2048], P(None, 'dp', 'tensor')
- head_bias_grad: float32 [3, 2048], P(None, 'tensor')
- dense_weight_grad: float32 [2048, 2048], P('tensor', 'dp')
- dense_bias_grad: float32 [2048], replicated
- fc1_weight_grad: float32 [2048, 8192], P('dp', 'tensor')
- fc1_bias_grad: float32 [8192], P('tensor')
- fc2_weight_grad: float32 [8192, 2048], P('tensor', 'dp')
- fc2_bias_grad: float32 [2048], replicated
- norm_gain_grad: float32 [2048], replicated
- norm_bias_grad: float32 [2048], replicated
The draws below stay inside these ranges and needn't reach their ends.
All inputs are finite; a program needn't handle non-finite values.
Results may differ from the reference program's by a relative error of at most 0.0095.
Values may be sent and summed in bfloat16 or wider, within the bound.
A program may use at most 256 MiB of HBM per device.

```python
import math
import jax
import jax.numpy as jnp
from jax import lax

D = 2048
HEADS = 32
HD = 64
ROT = 32
FF = 8192
SEQ_LEN = 1024
TOKENS = 8192


def raised(values, key, source, target, parts, factor):
    owner, partner = [(jnp.arange(values.shape[position]) // (values.shape[position] // parts)).reshape([-1 if axis == position else 1 for axis in range(values.ndim)]) for position in (source, target)]
    chosen = jax.random.permutation(key, parts)[partner]
    strong = (owner == chosen) | (owner == (partner + parts // 2) % parts)
    return jnp.where(strong, factor * values, values)


def block_scale(stream_key, shape, pieces, least, high):
    loudness, own = 1.0, jax.random.fold_in(stream_key, 6)
    for axis_at, blocks in pieces:
        draws = jnp.exp(jax.random.uniform(jax.random.fold_in(own, axis_at), (blocks,), jnp.float32, least / len(pieces), high / len(pieces)))
        loudness = loudness * jnp.repeat(draws, shape[axis_at] // blocks).reshape([-1 if axis == axis_at else 1 for axis in range(len(shape))])
    return loudness


def scatter_about(rng, extent, spread, bound, shards=(), held_as=jnp.bfloat16):
    values = jax.random.normal(rng, extent, jnp.float32) * spread
    if len(shards) > 0:
        values = block_scale(rng, extent, shards, -0.22, 0.18) * values
    return jnp.clip(values, min=-bound, max=bound).astype(held_as)


def bell_draw_with(stream_key, extent, deviation, limit, split, heavy, kind=jnp.bfloat16):
    entries = deviation * jax.random.normal(stream_key, extent, jnp.float32)
    if split:
        entries = entries * block_scale(stream_key, extent, split, -0.22, 0.18)
    return jnp.clip(raised(entries, jax.random.fold_in(stream_key, 3), *heavy), -limit, limit).astype(kind)


def setup_inputs(seed: int = 0) -> dict:
    splits = jax.random.split(jax.random.key(seed), 13)
    hidden_in = scatter_about(splits[0], (TOKENS, D), 1.0, 6.0, ((0, 32),))
    qkv_weight = scatter_about(splits[1], (3, D, D), D ** -0.5, 0.125, ((1, 8), (2, 4)))
    head_bias = scatter_about(splits[2], (3, D), 0.5, 3.0, ((1, 4),), jnp.float32)
    dense_weight = scatter_about(splits[3], (D, D), (D // 64) ** -0.5, 1.0, ((0, 4), (1, 8)))
    dense_bias = scatter_about(splits[4], (D,), 0.5, 3.0, (), jnp.float32)
    fc1_weight = scatter_about(splits[5], (D, FF), D ** -0.5, 0.125, ((0, 8), (1, 4)))
    fc1_bias = scatter_about(splits[6], (FF,), 0.5, 3.0, ((0, 4),), jnp.float32)
    fc2_weight = scatter_about(splits[7], (FF, D), FF ** -0.5, 0.0625, ((0, 4), (1, 8)))
    fc2_bias = scatter_about(splits[8], (D,), 0.5, 3.0, (), jnp.float32)
    norm_gain = jnp.clip(1.0 + 0.1 * jax.random.normal(splits[9], (D,), jnp.float32), 0.5, 1.5)
    norm_bias = scatter_about(splits[10], (D,), 0.3, 2.0, (), jnp.float32)
    out_grad = bell_draw_with(splits[11], (TOKENS, D), 1.0, 6.0, ((0, 32),), (0, 1, 32, 2.75))
    return {"hidden_in": hidden_in, "qkv_weight": qkv_weight, "head_bias": head_bias, "dense_weight": dense_weight, "dense_bias": dense_bias, "fc1_weight": fc1_weight, "fc1_bias": fc1_bias, "fc2_weight": fc2_weight, "fc2_bias": fc2_bias, "norm_gain": norm_gain, "norm_bias": norm_bias, "out_grad": out_grad}


@jax.custom_vjp
def low(v):
    return lax.optimization_barrier(v.astype(jnp.bfloat16)).astype(jnp.float32)

@jax.custom_vjp
def low_back(v):
    return v

def low_keep(v):
    return (low(v), None)

def low_pass(kept, grad):
    return (grad,)

def back_keep(v):
    return (v, None)

def back_low(kept, grad):
    return (low(grad),)
low.defvjp(low_keep, low_pass)
low_back.defvjp(back_keep, back_low)
highest = lax.Precision.HIGHEST

def matmul(left, right):
    return jnp.dot(left, right, precision=highest, preferred_element_type=jnp.float32)

def gelu_tanh(values):
    return 0.5 * values * (1.0 + jnp.tanh(0.7978845608028654 * (values + 0.044715 * values * values * values)))

def rotate(values, sign):
    length = values.shape[0]
    half = ROT // 2
    freqs = 1.0 / 10000.0 ** (jnp.arange(half, dtype=jnp.float32) * 2.0 / ROT)
    angles = jnp.arange(length, dtype=jnp.float32)[:, None] * freqs[None, :]
    cosine = jnp.cos(angles)[:, None, :]
    sine = sign * jnp.sin(angles)[:, None, :]
    first = values[..., :half]
    second = values[..., half:ROT]
    return jnp.concatenate([first * cosine - second * sine, second * cosine + first * sine, values[..., ROT:]], axis=-1)

def layer(inputs, qkv_w, head_b, dense_w, dense_b, fc1_w, fc1_b, fc2_w, fc2_b, gain, shift):
    length = inputs.shape[0]
    centred = inputs - lax.optimization_barrier(jnp.mean(inputs, axis=-1, keepdims=True))
    normed = centred * lax.rsqrt(lax.optimization_barrier(jnp.mean(centred * centred, axis=-1, keepdims=True)) + 1e-05) * gain + shift
    normed = low(normed)
    queries = low_back(matmul(normed, qkv_w[0]) + head_b[0])
    keys = low_back(matmul(normed, qkv_w[1]) + head_b[1])
    values = low(low_back(matmul(normed, qkv_w[2]) + head_b[2])).reshape(length, HEADS, HD)
    queries = low(rotate(queries.reshape(length, HEADS, HD), 1.0))
    keys = low(rotate(keys.reshape(length, HEADS, HD), 1.0))
    scale = 1.0 / math.sqrt(HD)
    scores = low_back(jnp.einsum('qhd,khd->hqk', queries, keys, precision=highest) * scale)
    causal = jnp.arange(length)[None, :] <= jnp.arange(length)[:, None]
    probs = jax.nn.softmax(jnp.where(causal[None], scores, -1e+30), axis=-1)
    mixed = jnp.einsum('hqk,khd->qhd', low(probs), values, precision=highest)
    mixed = low(low_back(mixed.reshape(length, D)))
    attention = matmul(mixed, dense_w) + dense_b
    hidden = low_back(matmul(normed, fc1_w) + fc1_b)
    feed = matmul(low(gelu_tanh(hidden)), fc2_w) + fc2_b
    return inputs + attention + feed

def reference(hidden_in, qkv_weight, head_bias, dense_weight, dense_bias, fc1_weight, fc1_bias, fc2_weight, fc2_bias, norm_gain, norm_bias, out_grad):
    params = tuple((param.astype(jnp.float32) for param in (qkv_weight, head_bias, dense_weight, dense_bias, fc1_weight, fc1_bias, fc2_weight, fc2_bias, norm_gain, norm_bias)))
    count = hidden_in.shape[0] // SEQ_LEN
    inputs = hidden_in.astype(jnp.float32).reshape(count, SEQ_LEN, D)
    cotangents = out_grad.astype(jnp.float32).reshape(count, SEQ_LEN, D)

    def step(totals, pair):
        seq_in, seq_grad = pair
        output, pullback = jax.vjp(layer, seq_in, *params)
        grads = pullback(seq_grad)
        totals = tuple((left + right for left, right in zip(totals, grads[1:])))
        return (totals, (output, grads[0]))
    zeros = tuple((jnp.zeros(param.shape, jnp.float32) for param in params))
    totals, (outputs, input_grads) = lax.scan(step, zeros, (inputs, cotangents))
    return (outputs.reshape(-1, D).astype(jnp.bfloat16), input_grads.reshape(-1, D).astype(jnp.bfloat16), totals[0], totals[1], totals[2], totals[3], totals[4], totals[5], totals[6], totals[7], totals[8], totals[9])
```

```python
import math

import jax
import jax.numpy as jnp
from jax import lax
from jax.sharding import PartitionSpec as P

HD = 64
ROT = 32
SEQ_LEN = 1024
LOW = jnp.bfloat16


def dot_right(left, right):
    return lax.dot_general(
        left, right, (((1,), (1,)), ((), ())), preferred_element_type=jnp.float32
    )


def dot_left(left, right):
    return lax.dot_general(
        left, right, (((0,), (0,)), ((), ())), preferred_element_type=jnp.float32
    )


def swap(value, axis, bit):
    size = lax.axis_size(axis)
    return lax.ppermute(value, axis, [(i, i ^ bit) for i in range(size)])


def outer_bits(size):
    return [1 << k for k in range(1, size.bit_length() - 1)]


def block_order(size):
    return list(range(0, size, 2)) + list(range(1, size, 2))


def halves(value, dim):
    middle = value.shape[dim] // 2
    return (
        lax.slice_in_dim(value, 0, middle, axis=dim),
        lax.slice_in_dim(value, middle, value.shape[dim], axis=dim),
    )


def gather_blocks(shard, dim):
    size = lax.axis_size("dp")
    blocks = {0: shard}
    bits = outer_bits(size)
    while bits:
        if len(bits) >= 2:
            one, two = bits[0], bits[1]
            bits = bits[2:]
            for offset, block in list(blocks.items()):
                by_one, by_two = swap(block, "dp", one), swap(block, "dp", two)
                far_low = swap(halves(by_one, dim)[0], "dp", two)
                far_high = swap(halves(by_two, dim)[1], "dp", one)
                blocks[offset ^ one] = by_one
                blocks[offset ^ two] = by_two
                blocks[offset ^ one ^ two] = jnp.concatenate([far_low, far_high], axis=dim)
        else:
            one = bits.pop()
            for offset, block in list(blocks.items()):
                blocks[offset ^ one] = swap(block, "dp", one)
    for offset, block in list(blocks.items()):
        blocks[offset ^ 1] = swap(block, "dp", 1)
    return jnp.concatenate([blocks[k] for k in block_order(size)], axis=dim)


def reduce_quad(own, first, second, far, one, two, dim):
    first_low, first_high = halves(first, dim)
    second_low, second_high = halves(second, dim)
    far_low, far_high = halves(far, dim)
    own_low, own_high = halves(own, dim)
    got_low = swap(jnp.concatenate([first_low, far_low], axis=dim).astype(LOW), "dp", one)
    got_high = swap(jnp.concatenate([second_high, far_high], axis=dim).astype(LOW), "dp", two)
    low_own, low_second = halves(got_low, dim)
    high_own, high_first = halves(got_high, dim)
    pass_low = swap(
        (second_low.astype(jnp.float32) + low_second.astype(jnp.float32)).astype(LOW), "dp", two
    )
    pass_high = swap(
        (first_high.astype(jnp.float32) + high_first.astype(jnp.float32)).astype(LOW), "dp", one
    )
    return jnp.concatenate(
        [
            own_low.astype(jnp.float32)
            + low_own.astype(jnp.float32)
            + pass_low.astype(jnp.float32),
            own_high.astype(jnp.float32)
            + high_own.astype(jnp.float32)
            + pass_high.astype(jnp.float32),
        ],
        axis=dim,
    )


def reduce_blocks(partial, dim):
    size = lax.axis_size("dp")
    received = swap(partial(1).astype(LOW), "dp", 1)
    summed = (partial(0) + received.astype(jnp.float32)).astype(LOW)
    offsets = list(range(0, size, 2))
    width = summed.shape[dim] // len(offsets)
    blocks = {
        offset: lax.slice_in_dim(summed, place * width, (place + 1) * width, axis=dim)
        for place, offset in enumerate(offsets)
    }
    bits = outer_bits(size)
    while bits:
        if len(bits) >= 2:
            one, two = bits[-2], bits[-1]
            bits = bits[:-2]
            for offset in [k for k in blocks if not k & (one | two)]:
                blocks[offset] = reduce_quad(
                    blocks[offset],
                    blocks[offset ^ one],
                    blocks[offset ^ two],
                    blocks[offset ^ one ^ two],
                    one,
                    two,
                    dim,
                )
            blocks = {k: block for k, block in blocks.items() if not k & (one | two)}
        else:
            one = bits.pop()
            for offset in [k for k in blocks if not k & one]:
                blocks[offset] = blocks[offset].astype(jnp.float32) + swap(
                    blocks[offset ^ one].astype(LOW), "dp", one
                ).astype(jnp.float32)
            blocks = {k: block for k, block in blocks.items() if not k & one}
    return blocks[0].astype(jnp.float32)


def sum_over(value, axes):
    for axis in axes:
        bit = 1
        while bit < lax.axis_size(axis):
            value = value + swap(value, axis, bit)
            bit *= 2
    return value


def to_blocks(values):
    size, me = lax.axis_size("dp"), lax.axis_index("dp")
    width = values.shape[1] // size
    return jnp.concatenate(
        [
            lax.dynamic_slice_in_dim(values, (me ^ offset) * width, width, axis=1)
            for offset in block_order(size)
        ],
        axis=1,
    )


def from_blocks(values):
    size, me = lax.axis_size("dp"), lax.axis_index("dp")
    width = values.shape[1] // size
    pieces = []
    for block in range(size):
        offset = me ^ block
        place = offset // 2 + (offset % 2) * (size // 2)
        pieces.append(lax.dynamic_slice_in_dim(values, place * width, width, axis=1))
    return jnp.concatenate(pieces, axis=1)


def gelu_tanh(values):
    return (
        0.5
        * values
        * (1.0 + jnp.tanh(0.7978845608028654 * (values + 0.044715 * values * values * values)))
    )


def rotate(values, sign):
    length = values.shape[0]
    half = ROT // 2
    freqs = 1.0 / 10000.0 ** (jnp.arange(half, dtype=jnp.float32) * 2.0 / ROT)
    positions = (jnp.arange(length) % SEQ_LEN).astype(jnp.float32)
    angles = positions[:, None] * freqs[None, :]
    cosine = jnp.cos(angles)[:, None, :]
    sine = sign * jnp.sin(angles)[:, None, :]
    first = values[..., :half]
    second = values[..., half:ROT]
    return jnp.concatenate(
        [first * cosine - second * sine, second * cosine + first * sine, values[..., ROT:]], axis=-1
    )


def masked_scores(queries, keys, start, finish, scale):
    scores = (
        jnp.einsum(
            "sqhd,skhd->shqk",
            queries[:, start:finish],
            keys[:, :finish],
            preferred_element_type=jnp.float32,
        )
        * scale
    )
    causal = jnp.arange(finish)[None, :] <= (jnp.arange(finish - start) + start)[:, None]
    return jnp.where(causal, scores, -1e30)


def attend(queries, keys, values):
    length = queries.shape[1]
    block = min(512, length)
    scale = 1.0 / math.sqrt(queries.shape[3])
    outputs = []
    logsums = []
    for block_index in range(length // block):
        start = block_index * block
        finish = start + block
        scores = masked_scores(queries, keys, start, finish, scale)
        largest = jnp.max(scores, axis=-1, keepdims=True)
        expos = jnp.exp(scores - largest)
        summed = jnp.sum(expos, axis=-1, keepdims=True)
        probs = (expos / summed).astype(jnp.bfloat16)
        outputs.append(
            jnp.einsum(
                "shqk,skhd->sqhd", probs, values[:, :finish], preferred_element_type=jnp.float32
            )
        )
        logsums.append((largest + jnp.log(summed))[..., 0])
    return (jnp.concatenate(outputs, axis=1), jnp.concatenate(logsums, axis=2))


def attend_back(queries, keys, values, grads_out, logsum):
    length = queries.shape[1]
    block = min(512, length)
    scale = 1.0 / math.sqrt(queries.shape[3])
    query_grads = []
    key_grad = jnp.zeros(keys.shape, jnp.float32)
    value_grad = jnp.zeros(values.shape, jnp.float32)
    for block_index in range(length // block):
        start = block_index * block
        finish = start + block
        scores = masked_scores(queries, keys, start, finish, scale)
        probs = jnp.exp(scores - logsum[:, :, start:finish, None])
        products = jnp.einsum(
            "sqhd,skhd->shqk",
            grads_out[:, start:finish],
            values[:, :finish],
            preferred_element_type=jnp.float32,
        )
        inner = jnp.sum(probs * products, axis=-1, keepdims=True)
        score_grad = (probs * (products - inner)).astype(jnp.bfloat16)
        query_grads.append(
            jnp.einsum(
                "shqk,skhd->sqhd", score_grad, keys[:, :finish], preferred_element_type=jnp.float32
            )
            * scale
        )
        key_grad = key_grad.at[:, :finish].add(
            jnp.einsum(
                "shqk,sqhd->skhd",
                score_grad,
                queries[:, start:finish],
                preferred_element_type=jnp.float32,
            )
            * scale
        )
        value_grad = value_grad.at[:, :finish].add(
            jnp.einsum(
                "shqk,sqhd->skhd",
                probs.astype(jnp.bfloat16),
                grads_out[:, start:finish],
                preferred_element_type=jnp.float32,
            )
        )
    return (jnp.concatenate(query_grads, axis=1), key_grad, value_grad)


def per_device(
    hidden_in,
    qkv_weight,
    head_bias,
    dense_weight,
    dense_bias,
    fc1_weight,
    fc1_bias,
    fc2_weight,
    fc2_bias,
    norm_gain,
    norm_bias,
    out_grad,
):
    depth, width_local = qkv_weight.shape[1], qkv_weight.shape[2]
    inputs = hidden_in.astype(jnp.float32)
    centred = inputs - jnp.mean(inputs, axis=-1, keepdims=True)
    inverse_std = lax.rsqrt(jnp.mean(centred * centred, axis=-1, keepdims=True) + 1e-05)
    standard = centred * inverse_std
    normed = (standard * norm_gain + norm_bias).astype(jnp.bfloat16)
    normed_all = lax.all_gather(to_blocks(normed), "tensor", axis=0, tiled=True)
    grad_all = lax.all_gather(to_blocks(out_grad), "tensor", axis=0, tiled=True)
    qkv_flat = jnp.swapaxes(qkv_weight, 0, 1).reshape(depth, 3 * width_local)
    qkv_full = gather_blocks(qkv_flat, 0)
    fc1_full = gather_blocks(fc1_weight, 0)
    dense_full = gather_blocks(dense_weight, 1)
    fc2_full = gather_blocks(fc2_weight, 1)
    rows, features = normed_all.shape
    half = features // 2
    count = rows // SEQ_LEN
    heads_local = width_local // HD

    def split_heads(values):
        return values.reshape(count, SEQ_LEN, heads_local, HD)

    def half_of(values, which):
        return values[:, which * half : (which + 1) * half]

    output_bias_grad = sum_over(
        jnp.sum(out_grad.astype(jnp.float32), axis=0, keepdims=True), ("dp", "tensor")
    )[0]
    projected = jnp.dot(normed_all, qkv_full, preferred_element_type=jnp.float32) + (
        head_bias.reshape(1, 3 * width_local)
    )
    queries = rotate(
        projected[:, :width_local].reshape(rows, heads_local, HD), 1.0
    ).astype(jnp.bfloat16)
    keys = rotate(
        projected[:, width_local : 2 * width_local].reshape(rows, heads_local, HD), 1.0
    ).astype(jnp.bfloat16)
    values = projected[:, 2 * width_local :].astype(jnp.bfloat16).reshape(rows, heads_local, HD)
    mixed, logsum = attend(split_heads(queries), split_heads(keys), split_heads(values))
    mixed = mixed.reshape(rows, width_local).astype(jnp.bfloat16)
    hidden = jnp.dot(normed_all, fc1_full, preferred_element_type=jnp.float32) + fc1_bias
    active = gelu_tanh(hidden).astype(jnp.bfloat16)
    partial_value = jnp.dot(mixed, dense_full, preferred_element_type=jnp.float32) + jnp.dot(
        active, fc2_full, preferred_element_type=jnp.float32
    )
    summed = lax.psum_scatter(
        partial_value.astype(LOW), "tensor", scatter_dimension=0, tiled=True
    )
    hidden_out = (
        inputs + from_blocks(summed).astype(jnp.float32) + dense_bias + fc2_bias
    ).astype(jnp.bfloat16)
    fc2_grad = reduce_blocks(lambda which: dot_left(active, half_of(grad_all, which)), 1)
    dense_grad = reduce_blocks(lambda which: dot_left(mixed, half_of(grad_all, which)), 1)
    feed_grad = dot_right(grad_all, fc2_full)
    unused, gelu_pull = jax.vjp(gelu_tanh, hidden)
    hidden_back = gelu_pull(feed_grad)[0].astype(jnp.bfloat16)
    fc1_grad = reduce_blocks(lambda which: dot_left(half_of(normed_all, which), hidden_back), 0)
    fc1_bias_part = jnp.sum(hidden_back.astype(jnp.float32), axis=0)
    mixed_back = dot_right(grad_all, dense_full).astype(jnp.bfloat16)
    query_back, key_back, value_back = attend_back(
        split_heads(queries),
        split_heads(keys),
        split_heads(values),
        split_heads(mixed_back),
        logsum,
    )
    query_back = rotate(query_back.reshape(rows, heads_local, HD), -1.0).reshape(rows, width_local)
    key_back = rotate(key_back.reshape(rows, heads_local, HD), -1.0).reshape(rows, width_local)
    proj_back = jnp.concatenate(
        [query_back, key_back, value_back.reshape(rows, width_local)], axis=1
    ).astype(jnp.bfloat16)
    normed_back = dot_right(hidden_back, fc1_full) + dot_right(proj_back, qkv_full)
    own_back = from_blocks(
        lax.psum_scatter(normed_back.astype(LOW), "tensor", scatter_dimension=0, tiled=True)
    ).astype(jnp.float32)
    qkv_grad = reduce_blocks(lambda which: dot_left(half_of(normed_all, which), proj_back), 0)
    qkv_grad = jnp.swapaxes(qkv_grad.reshape(depth, 3, width_local), 0, 1)
    head_bias_part = jnp.sum(proj_back.astype(jnp.float32), axis=0)
    bias_grads = sum_over(jnp.concatenate([head_bias_part, fc1_bias_part])[None], ("dp",))[0]
    head_bias_grad = bias_grads[: 3 * width_local].reshape(3, width_local)
    fc1_bias_grad = bias_grads[3 * width_local :]
    scaled = own_back * norm_gain
    hidden_grad = out_grad.astype(jnp.float32) + inverse_std * (
        scaled
        - jnp.mean(scaled, axis=-1, keepdims=True)
        - standard * jnp.mean(scaled * standard, axis=-1, keepdims=True)
    )
    norm_grads = sum_over(
        jnp.stack([jnp.sum(own_back * standard, axis=0), jnp.sum(own_back, axis=0)]),
        ("dp", "tensor"),
    )
    return (
        hidden_out,
        hidden_grad.astype(jnp.bfloat16),
        qkv_grad,
        head_bias_grad,
        dense_grad,
        output_bias_grad,
        fc1_grad,
        fc1_bias_grad,
        fc2_grad,
        output_bias_grad,
        norm_grads[0],
        norm_grads[1],
    )


def solution(mesh):
    placed = (
        P(("dp", "tensor"), None),
        P(None, "dp", "tensor"),
        P(None, "tensor"),
        P("tensor", "dp"),
        P(),
        P("dp", "tensor"),
        P("tensor"),
        P("tensor", "dp"),
        P(),
        P(),
        P(),
        P(("dp", "tensor"), None),
    )
    return jax.shard_map(
        per_device,
        mesh=mesh,
        in_specs=placed,
        out_specs=(
            P(("dp", "tensor"), None),
            P(("dp", "tensor"), None),
            P(None, "dp", "tensor"),
            P(None, "tensor"),
            P("tensor", "dp"),
            P(),
            P("dp", "tensor"),
            P("tensor"),
            P("tensor", "dp"),
            P(),
            P(),
            P(),
        ),
        check_vma=False,
    )
```

```python
import math

import jax
import jax.numpy as jnp
from jax import lax
from jax.experimental import pallas as pl
from jax.experimental.pallas import tpu as pltpu
from jax.sharding import PartitionSpec as P

HD = 64
PAIR = 128
ROT = 32
SEQ_LEN = 1024
LOW = jnp.bfloat16


def dot_right(left, right):
    return lax.dot_general(
        left, right, (((1,), (1,)), ((), ())), preferred_element_type=jnp.float32
    )


def dot_plain(left, right):
    return jnp.dot(left, right, preferred_element_type=jnp.float32)


def dot_left(left, right):
    return lax.dot_general(
        left, right, (((0,), (0,)), ((), ())), preferred_element_type=jnp.float32
    )


def swap(value, axis, bit):
    size = lax.axis_size(axis)
    return lax.ppermute(value, axis, [(i, i ^ bit) for i in range(size)])


def outer_bits(size):
    return [1 << k for k in range(1, size.bit_length() - 1)]


def block_order(size):
    return list(range(0, size, 2)) + list(range(1, size, 2))


def halves(value, dim):
    middle = value.shape[dim] // 2
    return (
        lax.slice_in_dim(value, 0, middle, axis=dim),
        lax.slice_in_dim(value, middle, value.shape[dim], axis=dim),
    )


def gather_blocks(shard, dim):
    size = lax.axis_size("dp")
    blocks = {0: shard}
    bits = outer_bits(size)
    while bits:
        if len(bits) >= 2:
            one, two = bits[0], bits[1]
            bits = bits[2:]
            for offset, block in list(blocks.items()):
                by_one, by_two = swap(block, "dp", one), swap(block, "dp", two)
                far_low = swap(halves(by_one, dim)[0], "dp", two)
                far_high = swap(halves(by_two, dim)[1], "dp", one)
                blocks[offset ^ one] = by_one
                blocks[offset ^ two] = by_two
                blocks[offset ^ one ^ two] = jnp.concatenate([far_low, far_high], axis=dim)
        else:
            one = bits.pop()
            for offset, block in list(blocks.items()):
                blocks[offset ^ one] = swap(block, "dp", one)
    for offset, block in list(blocks.items()):
        blocks[offset ^ 1] = swap(block, "dp", 1)
    marker = tuple(blocks[1 << k] for k in range(size.bit_length() - 1))
    return jnp.concatenate([blocks[k] for k in block_order(size)], axis=dim), marker


def reduce_quad(own, first, second, far, one, two, dim):
    first_low, first_high = halves(first, dim)
    second_low, second_high = halves(second, dim)
    far_low, far_high = halves(far, dim)
    own_low, own_high = halves(own, dim)
    got_low = swap(jnp.concatenate([first_low, far_low], axis=dim).astype(LOW), "dp", one)
    got_high = swap(jnp.concatenate([second_high, far_high], axis=dim).astype(LOW), "dp", two)
    low_own, low_second = halves(got_low, dim)
    high_own, high_first = halves(got_high, dim)
    pass_low = swap(
        (second_low.astype(jnp.float32) + low_second.astype(jnp.float32)).astype(LOW), "dp", two
    )
    pass_high = swap(
        (first_high.astype(jnp.float32) + high_first.astype(jnp.float32)).astype(LOW), "dp", one
    )
    return jnp.concatenate(
        [
            own_low.astype(jnp.float32)
            + low_own.astype(jnp.float32)
            + pass_low.astype(jnp.float32),
            own_high.astype(jnp.float32)
            + high_own.astype(jnp.float32)
            + pass_high.astype(jnp.float32),
        ],
        axis=dim,
    )


def reduce_blocks(partial, dim):
    size = lax.axis_size("dp")
    received = swap(partial(1).astype(LOW), "dp", 1)
    summed = (partial(0) + received.astype(jnp.float32)).astype(LOW)
    offsets = list(range(0, size, 2))
    width = summed.shape[dim] // len(offsets)
    blocks = {
        offset: lax.slice_in_dim(summed, place * width, (place + 1) * width, axis=dim)
        for place, offset in enumerate(offsets)
    }
    bits = outer_bits(size)
    while bits:
        if len(bits) >= 2:
            one, two = bits[-2], bits[-1]
            bits = bits[:-2]
            for offset in [k for k in blocks if not k & (one | two)]:
                blocks[offset] = reduce_quad(
                    blocks[offset],
                    blocks[offset ^ one],
                    blocks[offset ^ two],
                    blocks[offset ^ one ^ two],
                    one,
                    two,
                    dim,
                )
            blocks = {k: block for k, block in blocks.items() if not k & (one | two)}
        else:
            one = bits.pop()
            for offset in [k for k in blocks if not k & one]:
                blocks[offset] = blocks[offset].astype(jnp.float32) + swap(
                    blocks[offset ^ one].astype(LOW), "dp", one
                ).astype(jnp.float32)
            blocks = {k: block for k, block in blocks.items() if not k & one}
    return blocks[0].astype(jnp.float32)


def sum_over(value, axes):
    for axis in axes:
        bit = 1
        while bit < lax.axis_size(axis):
            value = value + swap(value, axis, bit)
            bit *= 2
    return value


def to_blocks(values):
    size, me = lax.axis_size("dp"), lax.axis_index("dp")
    width = values.shape[1] // size
    return jnp.concatenate(
        [
            lax.dynamic_slice_in_dim(values, (me ^ offset) * width, width, axis=1)
            for offset in block_order(size)
        ],
        axis=1,
    )


def from_blocks(values):
    size, me = lax.axis_size("dp"), lax.axis_index("dp")
    width = values.shape[1] // size
    pieces = []
    for block in range(size):
        offset = me ^ block
        place = offset // 2 + (offset % 2) * (size // 2)
        pieces.append(lax.dynamic_slice_in_dim(values, place * width, width, axis=1))
    return jnp.concatenate(pieces, axis=1)


def gelu_tanh(values):
    return (
        0.5
        * values
        * (1.0 + jnp.tanh(0.7978845608028654 * (values + 0.044715 * values * values * values)))
    )


def rope_tables(length):
    half = ROT // 2
    freqs = 1.0 / 10000.0 ** (jnp.arange(half, dtype=jnp.float32) * 2.0 / ROT)
    angles = jnp.arange(length, dtype=jnp.float32)[:, None] * freqs[None, :]
    cosine, sine = jnp.cos(angles), jnp.sin(angles)
    zeros = jnp.zeros((length, half), jnp.float32)
    rest = jnp.zeros((length, HD - ROT), jnp.float32)
    here = jnp.concatenate([cosine, cosine, rest + 1.0], axis=1)
    above = jnp.concatenate([-sine, zeros, rest], axis=1)
    below = jnp.concatenate([zeros, sine, rest], axis=1)
    return tuple(jnp.concatenate([table, table], axis=1) for table in (here, above, below))


def turn(values, here, above, below, sign):
    half = ROT // 2
    return values * here + sign * (
        pltpu.roll(values, PAIR - half, 1) * above + pltpu.roll(values, half, 1) * below
    )


def lanes_of(values, head):
    lane = lax.broadcasted_iota(jnp.int32, values.shape, 1)
    return jnp.where((lane >= HD) == (head == 1), values, jnp.zeros_like(values))


def triangle(scores):
    row = lax.broadcasted_iota(jnp.int32, scores.shape, 0)
    column = lax.broadcasted_iota(jnp.int32, scores.shape, 1)
    return jnp.where(column <= row, scores, -1e30)


def attend_kernel(proj_ref, here_ref, above_ref, below_ref, qkv_ref, mixed_ref, logsum_ref):
    length = proj_ref.shape[0]
    block = min(256, length)
    here, above, below = here_ref[...], above_ref[...], below_ref[...]
    scale = 1.0 / math.sqrt(HD)
    qkv_ref[:, :PAIR] = turn(proj_ref[:, :PAIR], here, above, below, 1.0).astype(LOW)
    qkv_ref[:, PAIR : 2 * PAIR] = turn(
        proj_ref[:, PAIR : 2 * PAIR], here, above, below, 1.0
    ).astype(LOW)
    qkv_ref[:, 2 * PAIR :] = proj_ref[:, 2 * PAIR :].astype(LOW)
    for start in range(0, length, block):
        finish = start + block
        queries = qkv_ref[start:finish, :PAIR]
        keys, values = qkv_ref[start:finish, PAIR : 2 * PAIR], qkv_ref[start:finish, 2 * PAIR :]
        mixed = jnp.zeros((block, PAIR), jnp.float32)
        logsum = jnp.zeros((block, PAIR), jnp.float32)
        for head in range(2):
            own = lanes_of(queries, head)
            near = triangle(dot_right(own, keys) * scale)
            largest = jnp.max(near, axis=1, keepdims=True)
            if start:
                past = dot_right(own, qkv_ref[:start, PAIR : 2 * PAIR]) * scale
                largest = jnp.maximum(largest, jnp.max(past, axis=1, keepdims=True))
            near = jnp.exp(near - largest)
            summed = jnp.sum(near, axis=1, keepdims=True)
            if start:
                past = jnp.exp(past - largest)
                summed = summed + jnp.sum(past, axis=1, keepdims=True)
            inverse = 1.0 / summed
            out = dot_plain((near * inverse).astype(LOW), values)
            if start:
                out = out + dot_plain((past * inverse).astype(LOW), qkv_ref[:start, 2 * PAIR :])
            mixed = mixed + lanes_of(out, head)
            logsum = logsum + lanes_of(
                jnp.broadcast_to(largest + jnp.log(summed), (block, PAIR)), head
            )
        mixed_ref[start:finish, :] = mixed.astype(LOW)
        logsum_ref[start:finish, :] = logsum


def attend(projected):
    rows, pairs = projected.shape[0], projected.shape[1] // (3 * PAIR)
    count = rows // SEQ_LEN
    tables = rope_tables(SEQ_LEN)
    whole = pl.BlockSpec((SEQ_LEN, PAIR), lambda s, p: (0, 0))
    return pl.pallas_call(
        attend_kernel,
        grid=(count, pairs),
        in_specs=[pl.BlockSpec((SEQ_LEN, 3 * PAIR), lambda s, p: (s, p)), whole, whole, whole],
        out_specs=[
            pl.BlockSpec((SEQ_LEN, 3 * PAIR), lambda s, p: (s, p)),
            pl.BlockSpec((SEQ_LEN, PAIR), lambda s, p: (s, p)),
            pl.BlockSpec((SEQ_LEN, PAIR), lambda s, p: (s, p)),
        ],
        out_shape=[
            jax.ShapeDtypeStruct((rows, pairs * 3 * PAIR), LOW),
            jax.ShapeDtypeStruct((rows, pairs * PAIR), LOW),
            jax.ShapeDtypeStruct((rows, pairs * PAIR), jnp.float32),
        ],
        cost_estimate=pl.CostEstimate(
            flops=rows * SEQ_LEN * pairs * PAIR * 8,
            bytes_accessed=rows * pairs * PAIR * 24,
            transcendentals=rows * SEQ_LEN * pairs,
        ),
        name="attend",
    )(projected, *tables)


def attend_back_kernel(
    qkv_ref, grad_ref, logsum_ref, here_ref, above_ref, below_ref, back_ref, bias_ref, keys_ref, values_ref
):
    length = qkv_ref.shape[0]
    block = min(256, length)
    scale = 1.0 / math.sqrt(HD)
    for start in range(0, length, block):
        finish = start + block
        queries = qkv_ref[start:finish, :PAIR]
        grads = grad_ref[start:finish, :]
        query_back = jnp.zeros((block, PAIR), jnp.float32)
        for head in range(2):
            own, own_grads = lanes_of(queries, head), lanes_of(grads, head)
            logsum = logsum_ref[start:finish, head * HD : head * HD + 1]
            parts = [(start, finish)] + ([(0, start)] if start else [])
            probs, products = [], []
            inner = 0.0
            for begin, end in parts:
                scores = dot_right(own, qkv_ref[begin:end, PAIR : 2 * PAIR]) * scale
                if begin == start:
                    scores = triangle(scores)
                prob = jnp.exp(scores - logsum)
                product = dot_right(own_grads, qkv_ref[begin:end, 2 * PAIR :])
                inner = inner + jnp.sum(prob * product, axis=1, keepdims=True)
                probs.append(prob)
                products.append(product)
            back = jnp.zeros((block, PAIR), jnp.float32)
            for (begin, end), prob, product in zip(parts, probs, products):
                score_back = (prob * (product - inner)).astype(LOW)
                back = back + dot_plain(score_back, qkv_ref[begin:end, PAIR : 2 * PAIR])
                key_part = dot_left(score_back, own)
                value_part = dot_left(prob.astype(LOW), own_grads)
                if begin == start and head == 0:
                    keys_ref[begin:end, :] = key_part
                    values_ref[begin:end, :] = value_part
                else:
                    keys_ref[begin:end, :] += key_part
                    values_ref[begin:end, :] += value_part
            query_back = query_back + lanes_of(back, head)
        back_ref[start:finish, :PAIR] = turn(
            query_back * scale,
            here_ref[start:finish, :],
            above_ref[start:finish, :],
            below_ref[start:finish, :],
            -1.0,
        ).astype(LOW)
    back_ref[:, PAIR : 2 * PAIR] = turn(
        keys_ref[...] * scale, here_ref[...], above_ref[...], below_ref[...], -1.0
    ).astype(LOW)
    back_ref[:, 2 * PAIR :] = values_ref[...].astype(LOW)
    total = jnp.sum(back_ref[...].astype(jnp.float32), axis=0, keepdims=True)
    bias_ref[...] = jnp.broadcast_to(total, bias_ref.shape)


def attend_back(qkv, grads, logsum):
    rows, pairs = qkv.shape[0], qkv.shape[1] // (3 * PAIR)
    count = rows // SEQ_LEN
    tables = rope_tables(SEQ_LEN)
    whole = pl.BlockSpec((SEQ_LEN, PAIR), lambda s, p: (0, 0))
    back, bias = pl.pallas_call(
        attend_back_kernel,
        grid=(count, pairs),
        in_specs=[
            pl.BlockSpec((SEQ_LEN, 3 * PAIR), lambda s, p: (s, p)),
            pl.BlockSpec((SEQ_LEN, PAIR), lambda s, p: (s, p)),
            pl.BlockSpec((SEQ_LEN, PAIR), lambda s, p: (s, p)),
            whole,
            whole,
            whole,
        ],
        out_specs=[
            pl.BlockSpec((SEQ_LEN, 3 * PAIR), lambda s, p: (s, p)),
            pl.BlockSpec((8, 3 * PAIR), lambda s, p: (s, p)),
        ],
        out_shape=[
            jax.ShapeDtypeStruct((rows, pairs * 3 * PAIR), LOW),
            jax.ShapeDtypeStruct((count * 8, pairs * 3 * PAIR), jnp.float32),
        ],
        scratch_shapes=[pltpu.VMEM((SEQ_LEN, PAIR), jnp.float32)] * 2,
        cost_estimate=pl.CostEstimate(
            flops=rows * SEQ_LEN * pairs * PAIR * 20,
            bytes_accessed=rows * pairs * PAIR * 20,
            transcendentals=rows * SEQ_LEN * pairs,
        ),
        name="attend_back",
    )(qkv, grads, logsum, *tables)
    return back, jnp.sum(bias.reshape(count, 8, -1)[:, 0], axis=0)


def line_gather(shard):
    size, me = lax.axis_size("tensor"), lax.axis_index("tensor")
    rows = shard.shape[0]
    right = left = shard
    rights, lefts = [], []
    for step in range(1, size):
        right = lax.ppermute(right, "tensor", [(i, i + 1) for i in range(step - 1, size - 1)])
        left = lax.ppermute(left, "tensor", [(i, i - 1) for i in range(1, size - step + 1)])
        rights.append(right)
        lefts.append(left)
    full = jnp.zeros((size * rows, shard.shape[1]), shard.dtype)
    full = lax.dynamic_update_slice_in_dim(full, shard, me * rows, axis=0)
    for back in range(1, size):
        piece = jnp.where(me >= back, rights[back - 1], lefts[size - back - 1])
        full = lax.dynamic_update_slice_in_dim(full, piece, ((me + size - back) % size) * rows, axis=0)
    return full, (right, left)


def device(dp, tensor):
    return {"dp": dp, "tensor": tensor}


def spread_kernel(line, weights, *refs):
    count = len(weights)
    shards, fulls = refs[: count + 1], refs[count + 1 : 2 * count + 2]
    own_sem, send_sem, recv_sem, line_send, line_recv = refs[2 * count + 2 :]
    dp, me = lax.axis_index("dp"), lax.axis_index("tensor")
    partners = {bit: device(dp ^ bit, me) for bit in (1, 2, 4)}
    up, down = device(dp, jnp.minimum(me + 1, line - 1)), device(dp, jnp.maximum(me - 1, 0))
    has_up, has_down = me < line - 1, me > 0

    barrier = pltpu.get_barrier_semaphore()
    for bit in (1, 2, 4):
        pl.semaphore_signal(barrier, inc=1, device_id=partners[bit])

    @pl.when(has_up)
    def _():
        pl.semaphore_signal(barrier, inc=1, device_id=up)

    @pl.when(has_down)
    def _():
        pl.semaphore_signal(barrier, inc=1, device_id=down)

    pl.semaphore_wait(barrier, 3 + has_up.astype(jnp.int32) + has_down.astype(jnp.int32))

    rows_ref, rows_full = shards[0], fulls[0]
    rows = rows_ref.shape[0]

    def rows_at(place):
        place = jnp.clip(place, 0, line - 1)
        return rows_full.at[pl.ds(pl.multiple_of(place * rows, rows), rows), :]

    def upward(step):
        source = rows_ref if step == 0 else rows_at(me - step)
        return pltpu.make_async_remote_copy(
            src_ref=source,
            dst_ref=rows_at(me - step),
            send_sem=line_send.at[0, step],
            recv_sem=line_recv.at[0, step],
            device_id=up,
        )

    def downward(step):
        source = rows_ref if step == 0 else rows_at(me + step)
        return pltpu.make_async_remote_copy(
            src_ref=source,
            dst_ref=rows_at(me + step),
            send_sem=line_send.at[1, step],
            recv_sem=line_recv.at[1, step],
            device_id=down,
        )

    def sends_up(step):
        return has_up & (me >= step)

    def sends_down(step):
        return has_down & (me + step <= line - 1)

    def line_start(step):
        @pl.when(sends_up(step))
        def _():
            upward(step).start()

        @pl.when(sends_down(step))
        def _():
            downward(step).start()

    def line_wait(step):
        @pl.when(me >= step + 1)
        def _():
            upward(step).wait_recv()

        @pl.when(me + step + 1 <= line - 1)
        def _():
            downward(step).wait_recv()

    def line_sent(step):
        @pl.when(sends_up(step))
        def _():
            upward(step).wait_send()

        @pl.when(sends_down(step))
        def _():
            downward(step).wait_send()

    def place(k, offset, part=None):
        shard, dim = shards[k + 1], weights[k]
        slot = offset // 2 + (offset % 2) * 4
        index = [pl.ds(0, extent) for extent in shard.shape]
        index[dim] = pl.ds(slot * shard.shape[dim], shard.shape[dim])
        if part is not None:
            middle = shard.shape[0] // 2
            start = middle * part + (slot * shard.shape[0] if dim == 0 else 0)
            index[0] = pl.ds(start, middle)
        return fulls[k + 1].at[tuple(index)]

    def hop(k, number, source, target, bit):
        return pltpu.make_async_remote_copy(
            src_ref=source,
            dst_ref=target,
            send_sem=send_sem.at[k, number],
            recv_sem=recv_sem.at[k, number],
            device_id=partners[bit],
        )

    hops = []
    for k in range(count):
        shard = shards[k + 1]
        hops.append(
            [
                hop(k, 0, shard, place(k, 2), 2),
                hop(k, 1, shard, place(k, 4), 4),
                hop(k, 2, shard, place(k, 1), 1),
                hop(k, 3, place(k, 2, 0), place(k, 6, 0), 4),
                hop(k, 4, place(k, 4, 1), place(k, 6, 1), 2),
                hop(k, 5, place(k, 2), place(k, 3), 1),
                hop(k, 6, place(k, 4), place(k, 5), 1),
                hop(k, 7, place(k, 6), place(k, 7), 1),
            ]
        )
    copies = [pltpu.make_async_copy(rows_ref, rows_at(me), own_sem.at[count])]
    copies += [pltpu.make_async_copy(shards[k + 1], place(k, 0), own_sem.at[k]) for k in range(count)]

    line_start(0)
    for k in range(count):
        hops[k][0].start()
        hops[k][1].start()
    for k in range(count):
        hops[k][2].start()
    for copy in copies:
        copy.start()

    def relay(k):
        hops[k][0].wait_recv()
        hops[k][3].start()
        hops[k][5].start()
        hops[k][1].wait_recv()
        hops[k][4].start()
        hops[k][6].start()

    def finish(k):
        hops[k][3].wait_recv()
        hops[k][4].wait_recv()
        hops[k][7].start()

    for step in range(max(line - 1, count)):
        if step < count:
            relay(step)
        if step < line - 1:
            line_wait(step)
            if step + 1 < line - 1:
                line_start(step + 1)
    for k in range(count):
        finish(k)
    for k in range(count):
        for number in (2, 5, 6, 7):
            hops[k][number].wait_recv()
        for number in range(8):
            hops[k][number].wait_send()
    for step in range(line - 1):
        line_sent(step)
    for copy in copies:
        copy.wait()


def spread(shard, weights, dims):
    line = lax.axis_size("tensor")
    size = lax.axis_size("dp")
    if size != 8 or line < 2:
        return [line_gather(shard)[0]] + [
            gather_blocks(weight, dim)[0] for weight, dim in zip(weights, dims)
        ]

    def grown(value, dim, times):
        shape = list(value.shape)
        shape[dim] *= times
        return jax.ShapeDtypeStruct(tuple(shape), value.dtype)

    count = len(weights)
    return pl.pallas_call(
        lambda *refs: spread_kernel(line, dims, *refs),
        in_specs=[pl.BlockSpec(memory_space=pltpu.VMEM)] * (count + 1),
        out_specs=[pl.BlockSpec(memory_space=pl.ANY)] * (count + 1),
        out_shape=[grown(shard, 0, line)]
        + [grown(weight, dim, size) for weight, dim in zip(weights, dims)],
        scratch_shapes=[
            pltpu.SemaphoreType.DMA((count + 1,)),
            pltpu.SemaphoreType.DMA((count, 8)),
            pltpu.SemaphoreType.DMA((count, 8)),
            pltpu.SemaphoreType.DMA((2, line)),
            pltpu.SemaphoreType.DMA((2, line)),
        ],
        compiler_params=pltpu.CompilerParams(collective_id=0, has_side_effects=True),
        name="spread",
    )(shard, *weights)


def wait_for(value, marker):
    return lax.optimization_barrier((value, marker))[0]


def to_groups(values, dim):
    shape = values.shape
    split = shape[:dim] + (3, shape[dim] // (3 * PAIR), PAIR) + shape[dim + 1 :]
    return jnp.swapaxes(values.reshape(split), dim, dim + 1).reshape(shape)


def from_groups(values, dim):
    shape = values.shape
    split = shape[:dim] + (shape[dim] // (3 * PAIR), 3, PAIR) + shape[dim + 1 :]
    return jnp.swapaxes(values.reshape(split), dim, dim + 1).reshape(shape)


def per_device(
    hidden_in,
    qkv_weight,
    head_bias,
    dense_weight,
    dense_bias,
    fc1_weight,
    fc1_bias,
    fc2_weight,
    fc2_bias,
    norm_gain,
    norm_bias,
    out_grad,
):
    depth, width_local = qkv_weight.shape[1], qkv_weight.shape[2]
    inputs = hidden_in.astype(jnp.float32)
    centred = inputs - jnp.mean(inputs, axis=-1, keepdims=True)
    inverse_std = lax.rsqrt(jnp.mean(centred * centred, axis=-1, keepdims=True) + 1e-05)
    standard = centred * inverse_std
    normed = (standard * norm_gain + norm_bias).astype(jnp.bfloat16)
    qkv_flat = to_groups(jnp.swapaxes(qkv_weight, 0, 1).reshape(depth, 3 * width_local), 1)
    normed_all, qkv_full, fc1_full, dense_full = spread(
        to_blocks(normed), [qkv_flat, fc1_weight, dense_weight], (0, 0, 1)
    )
    grad_all = lax.all_gather(
        wait_for(to_blocks(out_grad), normed_all), "tensor", axis=0, tiled=True
    )
    fc2_full, unused = gather_blocks(wait_for(fc2_weight, normed_all), 1)
    rows, features = normed_all.shape
    half = features // 2

    def half_of(values, which):
        return values[:, which * half : (which + 1) * half]

    output_bias_grad = sum_over(
        jnp.sum(out_grad.astype(jnp.float32), axis=0, keepdims=True), ("dp", "tensor")
    )[0]
    projected = dot_plain(normed_all, qkv_full) + to_groups(head_bias.reshape(1, -1), 1)
    qkv, mixed, logsum = attend(projected)
    hidden = dot_plain(normed_all, fc1_full) + fc1_bias
    active = gelu_tanh(hidden).astype(LOW)
    partial_value = dot_plain(mixed, dense_full) + dot_plain(active, fc2_full)
    summed = lax.psum_scatter(
        partial_value.astype(LOW), "tensor", scatter_dimension=0, tiled=True
    )
    hidden_out = (inputs + from_blocks(summed).astype(jnp.float32) + dense_bias + fc2_bias).astype(LOW)
    fc2_grad = reduce_blocks(lambda which: dot_left(active, half_of(grad_all, which)), 1)
    dense_grad = reduce_blocks(lambda which: dot_left(mixed, half_of(grad_all, which)), 1)
    feed_grad = dot_right(grad_all, fc2_full)
    unused, gelu_pull = jax.vjp(gelu_tanh, hidden)
    hidden_back = gelu_pull(feed_grad)[0].astype(LOW)
    fc1_grad = reduce_blocks(lambda which: dot_left(half_of(normed_all, which), hidden_back), 0)
    fc1_bias_part = jnp.sum(hidden_back.astype(jnp.float32), axis=0)
    mixed_back = dot_right(grad_all, dense_full).astype(LOW)
    proj_back, head_bias_part = attend_back(qkv, mixed_back, logsum)
    normed_back = dot_right(hidden_back, fc1_full) + dot_right(proj_back, qkv_full)
    own_back = from_blocks(
        lax.psum_scatter(normed_back.astype(LOW), "tensor", scatter_dimension=0, tiled=True)
    ).astype(jnp.float32)
    qkv_grad = reduce_blocks(lambda which: dot_left(half_of(normed_all, which), proj_back), 0)
    qkv_grad = jnp.swapaxes(from_groups(qkv_grad, 1).reshape(depth, 3, width_local), 0, 1)
    bias_grads = sum_over(
        jnp.concatenate([from_groups(head_bias_part, 0), fc1_bias_part])[None], ("dp",)
    )[0]
    head_bias_grad = bias_grads[: 3 * width_local].reshape(3, width_local)
    fc1_bias_grad = bias_grads[3 * width_local :]
    scaled = own_back * norm_gain
    hidden_grad = out_grad.astype(jnp.float32) + inverse_std * (
        scaled
        - jnp.mean(scaled, axis=-1, keepdims=True)
        - standard * jnp.mean(scaled * standard, axis=-1, keepdims=True)
    )
    norm_grads = sum_over(
        jnp.stack([jnp.sum(own_back * standard, axis=0), jnp.sum(own_back, axis=0)]),
        ("dp", "tensor"),
    )
    return (
        hidden_out,
        hidden_grad.astype(jnp.bfloat16),
        qkv_grad,
        head_bias_grad,
        dense_grad,
        output_bias_grad,
        fc1_grad,
        fc1_bias_grad,
        fc2_grad,
        output_bias_grad,
        norm_grads[0],
        norm_grads[1],
    )


def solution(mesh):
    placed = (
        P(("dp", "tensor"), None),
        P(None, "dp", "tensor"),
        P(None, "tensor"),
        P("tensor", "dp"),
        P(),
        P("dp", "tensor"),
        P("tensor"),
        P("tensor", "dp"),
        P(),
        P(),
        P(),
        P(("dp", "tensor"), None),
    )
    return jax.shard_map(
        per_device,
        mesh=mesh,
        in_specs=placed,
        out_specs=(
            P(("dp", "tensor"), None),
            P(("dp", "tensor"), None),
            P(None, "dp", "tensor"),
            P(None, "tensor"),
            P("tensor", "dp"),
            P(),
            P("dp", "tensor"),
            P("tensor"),
            P("tensor", "dp"),
            P(),
            P(),
            P(),
        ),
        check_vma=False,
    )
```
